32 devices in a mesh: dp: 8 (over y, x, core), mp: 4 (over z).
Axes of the slice: x: 2, y: 2, z: 4, core: 2. Of those that a mesh axis runs over, the one named last changes fastest.
Arguments:
- acts: bfloat16 [4096, 3072], P('dp'), may hold values from -16 to 16
- grads_out: bfloat16 [4096, 8192], P('dp', 'mp'), may hold values from -0.125 to 0.125
- old_a: float32 [8, 3, 128, 1024], P('dp'), may hold values from -0.09375 to 0.09375
- old_g: float32 [4, 8, 2, 128, 1024], P('mp', 'dp'), may hold values from -0.09375 to 0.09375
- a_inverse: bfloat16 [3072, 1024], P('dp'), may hold values from -0.1875 to 0.1875
- g_inverse: bfloat16 [8192, 1024], P('mp'), may hold values from -0.1875 to 0.1875
- owner_map: int32 [5, 8], replicated, may hold values from 0 to 7, each once within a row
Outputs:
- a_factor: float32 [8, 3, 128, 1024], P('dp')
- g_factor: float32 [4, 8, 2, 128, 1024], P('mp', 'dp')
- preconditioned: bfloat16 [3072, 4, 2048], P(None, 'mp', 'dp')
The draws below stay inside these ranges and needn't reach their ends.
Inputs may be any that keep to these rules, and one draw needn't show every extreme that they name: `owner_map`: each row is a permutation: row k tells, for each of the 8 row strips of factor block k, which dp index holds it. Rows 0 to 2 are the activation blocks, the others the output-gradient blocks of every mp index.
All inputs are finite; a program needn't handle non-finite values.
Results may differ from the reference program's by a relative error of at most 0.02.
Values may be sent and summed in bfloat16 or wider, within the bound.
A program may use at most 128 MiB of HBM per device.

```python
import jax
import jax.numpy as jnp
from jax import lax

D_WIN = 3072
BLOCK = 1024
FF_DEV = 2048
TOK_DEV = 512
TOKENS = 4096
FF_WIN = 8192
NA = 3
NG = 2
STRIP = 128
N_DP = 8
N_MP = 4


def draw_acts(key, part):
    values = jnp.clip(jax.random.normal(jax.random.fold_in(key, 23), (TOKENS, D_WIN), jnp.float32), -5.0, 5.0)
    pairing = jax.random.permutation(jax.random.fold_in(key, 29), N_DP)
    token_block = jnp.arange(TOKENS, dtype=jnp.int32) // TOK_DEV
    feature_block = jnp.arange(D_WIN, dtype=jnp.int32) // (D_WIN // N_DP)
    paired = pairing[token_block][:, None] == feature_block[None, :]
    return jnp.where(paired, 3.0 * values, values).astype(jnp.bfloat16)


def draw_grads_out(key, part):
    spread = TOKENS ** (-0.5)
    values = jnp.clip(jax.random.normal(jax.random.fold_in(key, 37), (TOKENS, FF_WIN), jnp.float32), -6.0, 6.0)
    return (values * spread).astype(jnp.bfloat16)


def levels(own_key, shape, shards, smallest, top_value):
    def one(position, shards_of):
        steps = jax.random.uniform(jax.random.fold_in(jax.random.fold_in(own_key, 6), position), (shards_of,), jnp.float32, smallest / len(shards), top_value / len(shards))
        return jnp.repeat(jnp.exp(steps), shape[position] // shards_of).reshape((-1,) + (1,) * (len(shape) - position - 1))

    loudness = one(*shards[0])
    for cut in shards[1:]:
        loudness = loudness * one(*cut)
    return loudness


def normal_values(key, extent, scale, limit, shards=(), held_as=jnp.bfloat16):
    entries = jax.random.normal(key, extent, jnp.float32) * scale
    if len(shards) > 0:
        entries = levels(key, extent, shards, -0.22, 0.18) * entries
    return jnp.clip(entries, min=-limit, max=limit).astype(held_as)


def setup_inputs(seed: int = 0) -> dict:
    arg_keys = jax.random.split(jax.random.key(seed), 8)
    acts = draw_acts(jax.random.fold_in(arg_keys[7], 71), 0)
    grads_out = draw_grads_out(jax.random.fold_in(arg_keys[7], 71), 0)
    old_a = normal_values(arg_keys[2], (N_DP, NA, STRIP, BLOCK), (TOKENS ** -0.5), 0.09375, ((0, 8),), jnp.float32)
    old_g = normal_values(arg_keys[3], (N_MP, N_DP, NG, STRIP, BLOCK), (TOKENS ** -0.5), 0.09375, ((0, 4), (1, 8)), jnp.float32)
    a_inverse = normal_values(arg_keys[4], (D_WIN, BLOCK), BLOCK ** -0.5, 0.1875, ((0, 8),))
    g_inverse = normal_values(arg_keys[5], (FF_WIN, BLOCK), BLOCK ** -0.5, 0.1875, ((0, 4),))
    owner_map = jax.vmap(lambda own: jax.random.permutation(own, N_DP))(jax.random.split(arg_keys[6], (NA + NG))).reshape((NA + NG, N_DP)).astype(jnp.int32)
    return {"acts": acts, "grads_out": grads_out, "old_a": old_a, "old_g": old_g, "a_inverse": a_inverse, "g_inverse": g_inverse, "owner_map": owner_map}


decay_rate = 0.75


def accumulate(running, pieces):
    act_rows, grad_rows = pieces
    act_blocks = act_rows.reshape(TOK_DEV, NA, BLOCK).astype(jnp.float32)
    grad_blocks = grad_rows.reshape(TOK_DEV, N_MP * NG, BLOCK).astype(jnp.float32)
    act_cov = jnp.einsum('tkb,tkc->kbc', act_blocks, act_blocks) / (TOK_DEV * N_DP)
    grad_cov = jnp.einsum('tkb,tkc->kbc', grad_blocks, grad_blocks)
    partial_grad = jnp.dot(act_rows.T, grad_rows, preferred_element_type=jnp.float32).astype(jnp.bfloat16)
    partial_grad = lax.optimization_barrier(partial_grad).astype(jnp.float32)
    return (running[0] + act_cov, running[1] + grad_cov, running[2] + partial_grad), None


def reference(acts, grads_out, old_a, old_g, a_inverse, g_inverse, owner_map):
    acts_split = acts.reshape(N_DP, TOK_DEV, D_WIN)
    grads_split = grads_out.reshape(N_DP, TOK_DEV, FF_WIN)
    start_state = (jnp.zeros((NA, BLOCK, BLOCK), jnp.float32),
                   jnp.zeros((N_MP * NG, BLOCK, BLOCK), jnp.float32),
                   jnp.zeros((D_WIN, FF_WIN), jnp.float32))
    final, unused = lax.scan(accumulate, start_state, (acts_split, grads_split))
    cov_a = final[0]
    cov_g = final[1]
    grad_sum = final[2]
    owners = jnp.arange(N_DP, dtype=jnp.int32)
    onehot = (owner_map[:, :, None] == owners[None, None, :]).astype(jnp.float32)
    a_strips = cov_a.reshape(NA, N_DP, STRIP, BLOCK)
    a_owned = jnp.einsum('ksd,ksrc->dkrc', onehot[:NA], a_strips, precision=lax.Precision.HIGHEST)
    g_strips = cov_g.reshape(N_MP, NG, N_DP, STRIP, BLOCK)
    g_owned = jnp.einsum('jsd,mjsrc->mdjrc', onehot[NA:], g_strips, precision=lax.Precision.HIGHEST)
    a_factor = decay_rate * old_a + (1.0 - decay_rate) * a_owned
    g_factor = decay_rate * old_g + (1.0 - decay_rate) * g_owned
    grad_low = grad_sum.astype(jnp.bfloat16).astype(jnp.float32)
    g_blocks = g_inverse.reshape(N_MP * NG, BLOCK, BLOCK).astype(jnp.float32)
    right_done = jnp.einsum('rjb,jbc->rjc', grad_low.reshape(D_WIN, N_MP * NG, BLOCK), g_blocks)
    right_done = right_done.astype(jnp.bfloat16).astype(jnp.float32).reshape(NA, BLOCK, FF_WIN)
    a_blocks = a_inverse.reshape(NA, BLOCK, BLOCK).astype(jnp.float32)
    result = jnp.einsum('kbc,kcf->kbf', a_blocks, right_done).astype(jnp.bfloat16)
    return a_factor, g_factor, result.reshape(D_WIN, N_MP, FF_DEV)
```

```python
import jax
import jax.numpy as jnp
from jax import lax
from jax.sharding import PartitionSpec as P

decay_rate = 0.75


def side_of(bit):
    hop = 2 << bit
    pairs = [(i, i ^ hop) for i in range(lax.axis_size("dp"))]
    return pairs, lax.rem(lax.axis_index("dp") // hop, 2)


def split_at(strips, bit):
    unused, mine = side_of(bit)
    chips, rows, columns = strips.shape
    strips = strips.reshape(chips >> (bit + 1), 2, 1 << bit, rows, columns)
    return [
        lax.dynamic_index_in_dim(strips, side, 1, keepdims=False).reshape(-1, rows, columns)
        for side in (1 - mine, mine)
    ]


def multiply_split(turned, acts, bit):
    unused, mine = side_of(bit)
    tokens, chips, width = turned.shape
    turned = turned.reshape(tokens, chips >> (bit + 1), 2, 1 << bit, width)
    parts = []
    for side in (1 - mine, mine):
        cols = lax.dynamic_index_in_dim(turned, side, 2, keepdims=False).reshape(tokens, -1)
        part = lax.dot_general(
            cols, acts, (((0,), (0,)), ((), ())), preferred_element_type=jnp.float32
        )
        parts.append(part.astype(jnp.bfloat16).reshape(chips // 2, width, -1))
    return parts


def halve(parts, order, after=None):
    away, kept = parts
    done = []
    for place, bit in enumerate(order):
        came = lax.ppermute(away, "dp", side_of(bit)[0])
        if place == 0 and after is not None:
            came, unused = lax.optimization_barrier((came, after))
        total = (kept.astype(jnp.float32) + came.astype(jnp.float32)).astype(jnp.bfloat16)
        done.append(bit)
        if place + 1 < len(order):
            later = order[place + 1]
            lower = later - sum(1 for old in done if old < later)
            away, kept = split_between(total, lower, later)
    return total.reshape(total.shape[1:])


def split_between(total, place, bit):
    unused, mine = side_of(bit)
    count, rows, columns = total.shape
    total = total.reshape(count >> (place + 1), 2, 1 << place, rows, columns)
    return [
        lax.dynamic_index_in_dim(total, side, 1, keepdims=False).reshape(-1, rows, columns)
        for side in (1 - mine, mine)
    ]


def gather_mp(mine):
    mp_count = lax.axis_size("mp")
    me = lax.axis_index("mp")
    rows = [mine]
    for step in range(1, mp_count):
        rows.append(lax.ppermute(mine, "mp", [(i, (i + step) % mp_count) for i in range(mp_count)]))
    rows = jnp.concatenate(rows, axis=1)
    source = lax.rem(me - jnp.arange(mp_count, dtype=jnp.int32) + mp_count, mp_count)
    return rows.at[:, source].get(mode="promise_in_bounds")


def per_device(acts, grads_out, old_a, old_g, a_inverse, g_inverse, owner_map):
    dp_count = lax.axis_size("dp")
    mp_count = lax.axis_size("mp")
    core = lax.rem(lax.axis_index("dp"), 2)
    chips = dp_count // 2
    features = acts.shape[1]
    hidden = grads_out.shape[1]
    block = a_inverse.shape[1]
    na = features // block
    ng = hidden // block
    tokens = acts.shape[0] * dp_count
    strip = block // dp_count
    sub = strip // mp_count
    width = hidden // dp_count
    pairs = [(i, i + 1 - 2 * (i % 2)) for i in range(dp_count)]

    bits = list(range(chips.bit_length() - 1))
    inverse_all = lax.all_gather(a_inverse, "dp", axis=0, tiled=True).reshape(na, block, block)

    other_acts = lax.ppermute(acts, "dp", pairs)
    turned = jnp.einsum(
        "tjb,jbc->tjc",
        grads_out.reshape(-1, ng, block),
        g_inverse.reshape(ng, block, block),
        preferred_element_type=jnp.float32,
    )
    turned = turned.astype(jnp.bfloat16).reshape(-1, chips, 2, width)
    turned_kept = lax.dynamic_index_in_dim(turned, core, 2, keepdims=False)
    turned_sent = lax.dynamic_index_in_dim(turned, 1 - core, 2, keepdims=False)
    turned = jnp.concatenate([turned_kept, lax.ppermute(turned_sent, "dp", pairs)], axis=0)
    acts2 = jnp.concatenate([acts, other_acts], axis=0)
    half = features // 2
    first = multiply_split(turned, acts2[:, :half], bits[0])
    second = multiply_split(turned, acts2[:, half:], bits[-1])
    grads_out, acts2, unused = lax.optimization_barrier((grads_out, acts2, (first[0], second[0])))

    other_grads = lax.ppermute(grads_out, "dp", pairs)
    grads2 = jnp.concatenate([grads_out, other_grads], axis=0)

    owners = jnp.arange(dp_count, dtype=jnp.int32)
    matches = owner_map[:, :, None] == owners[None, None, :]
    where_from = jnp.sum(jnp.where(matches, owners[None, :, None], 0), axis=1)
    mine = lax.dynamic_index_in_dim(where_from.reshape(na + ng, chips, 2), core, 2, keepdims=False)
    blocks_g = grads2.reshape(-1, ng, block)
    blocks_a = acts2.reshape(-1, na, block)
    g_partial = jnp.einsum("tkb,tkc->kbc", blocks_g, blocks_g, preferred_element_type=jnp.float32)
    g_partial = g_partial.astype(jnp.bfloat16).reshape(ng * dp_count, strip, block)
    own_rows = lax.dynamic_index_in_dim(
        blocks_a.reshape(-1, na, dp_count, mp_count, sub), lax.axis_index("mp"), 3, keepdims=False
    )
    a_partial = (
        jnp.einsum("tksr,tkc->ksrc", own_rows, blocks_a, preferred_element_type=jnp.float32)
        / tokens
    )
    a_partial = a_partial.astype(jnp.bfloat16).reshape(na * dp_count, sub, block)
    pick_a = (mine[:na] + dp_count * jnp.arange(na, dtype=jnp.int32)[:, None]).T.reshape(-1)
    pick_g = (mine[na:] + dp_count * jnp.arange(ng, dtype=jnp.int32)[:, None]).T.reshape(-1)
    g_sent = g_partial.at[pick_g].get(mode="promise_in_bounds").reshape(chips, ng * strip, block)
    a_sent = a_partial.at[pick_a].get(mode="promise_in_bounds").reshape(chips, na * sub, block)
    sent = jnp.concatenate([g_sent, a_sent], axis=1)
    right = jnp.concatenate([halve(first, bits, sent), halve(second, bits[::-1], sent)], axis=1)
    cut = block // 2
    cov = jnp.concatenate(
        [
            halve(split_at(sent[:, :, :cut], bits[0]), bits),
            halve(split_at(sent[:, :, cut:], bits[-1]), bits[::-1]),
        ],
        axis=1,
    )
    result = jnp.einsum(
        "kbc,wkc->kbw",
        inverse_all,
        right.reshape(width, na, block),
        preferred_element_type=jnp.float32,
    )
    cov, result = lax.optimization_barrier((cov, result.astype(jnp.bfloat16)))
    g_cov = cov[: ng * strip].astype(jnp.float32)
    a_cov = gather_mp(cov[ng * strip :].reshape(na, 1, sub, block))
    g_factor = decay_rate * old_g + (1.0 - decay_rate) * g_cov.reshape(old_g.shape)
    a_factor = decay_rate * old_a + (1.0 - decay_rate) * a_cov.astype(jnp.float32).reshape(old_a.shape)

    return (a_factor, g_factor, result.reshape(features, 1, width))


def solution(mesh):
    placed = (
        P("dp", None),
        P("dp", "mp"),
        P("dp", None, None, None),
        P("mp", "dp", None, None, None),
        P("dp", None),
        P("mp", None),
        P(),
    )
    return jax.shard_map(
        per_device,
        mesh=mesh,
        in_specs=placed,
        out_specs=(P("dp", None, None, None), P("mp", "dp", None, None, None), P(None, "mp", "dp")),
        check_vma=False,
    )
```
